32 devices in a mesh: ctx: 16 (over z, y, x), tp: 2 (over core).
Axes of the slice: x: 2, y: 2, z: 4, core: 2. Of those that a mesh axis runs over, the one named last changes fastest.
Arguments:
- byte_states: bfloat16 [4096, 1024], P('ctx'), may hold values from -12 to 12, as said below
- patch_of_byte: int32 [4096], P('ctx'), may hold values from 0 to 125, as said below
- patch_first: int32 [16], replicated, may hold values from 0 to 991, as said below
- moved: int32 [2, 16], replicated, may hold values from 0 to 32, as said below
- w_qkv: bfloat16 [3, 1024, 2048], P(None, None, 'tp'), may hold values from -0.25 to 0.25, as said below
- d_attn: bfloat16 [1024, 2048], P('ctx', 'tp'), may hold values from -6 to 6
Outputs:
- attn_out: bfloat16 [1024, 2048], P('ctx', 'tp')
- byte_grad: bfloat16 [4096, 1024], P('ctx', 'tp')
The draws below stay inside these ranges and needn't reach their ends.
Inputs may be any that keep to these rules, and one draw needn't show every extreme that they name: `patch_of_byte`: within each byte shard the numbers start at 0 and rise by 0 or 1 from byte to byte; a shard holds at most 126 patches, reached on some shard. `patch_first`: the sum of the patch counts of all earlier byte shards; shard 0 starts at 0. moved[0, 0] = 0 and moved[1, 15] = 0; every other entry is 1 to 32; every patch shard thereby receives exactly 64 patches, and the patch counts agree with patch_first and patch_of_byte. `w_qkv`: independent entries of order 1024 ** -0.5. `byte_states`: entries of order one.
All inputs are finite; a program needn't handle non-finite values.
Results may differ from the reference program's by a relative error of at most 0.011.
Values may be sent and summed in bfloat16 or wider, within the bound.
A program may use at most 64 MiB of HBM per device.

```python
import jax
import jax.numpy as jnp
from jax import lax

DL = 1024
HEADS = 16
HD = 128
P_DEV = 64
BYTE_DEV = 256
KEYS = 1024
BYTES = 4096
N_CTX = 16


def shard_plan(key):
    reach = P_DEV // 2
    lower_moves = jax.random.randint(jax.random.fold_in(key, 11), (N_CTX,), 1, reach + 1)
    upper_moves = jax.random.randint(jax.random.fold_in(key, 13), (N_CTX,), 1, reach + 1)
    chosen = jax.random.randint(jax.random.fold_in(key, 17), (), 1, N_CTX - 1)
    place = jnp.arange(N_CTX)
    lower_moves = jnp.where(place == chosen, reach, lower_moves)
    upper_moves = jnp.where(place == chosen, reach, upper_moves)
    upper_moves = jnp.where(place == chosen - 1, 1, upper_moves)
    lower_moves = jnp.where(place == chosen + 1, 1, lower_moves)
    lower_moves = jnp.where(place == 0, 0, lower_moves)
    upper_moves = jnp.where(place == N_CTX - 1, 0, upper_moves)
    below_high = jnp.concatenate([jnp.zeros((1,), jnp.int32), upper_moves[:-1]])
    above_low = jnp.concatenate([lower_moves[1:], jnp.zeros((1,), jnp.int32)])
    counts = P_DEV - below_high - above_low + lower_moves + upper_moves
    return (counts.astype(jnp.int32), lower_moves.astype(jnp.int32), upper_moves.astype(jnp.int32))


def draw_patch_first(key, part):
    counts, lower_moves, upper_moves = shard_plan(key)
    return (jnp.cumsum(counts) - counts).astype(jnp.int32)


def draw_moved(key, part):
    counts, lower_moves, upper_moves = shard_plan(key)
    return jnp.stack([lower_moves, upper_moves], axis=0).astype(jnp.int32)


def draw_patch_of_byte(key, part):
    counts, lower_moves, upper_moves = shard_plan(key)
    shard_keys = jax.random.split(jax.random.fold_in(key, 23), N_CTX)

    def one_shard(shard_key, count):
        order = jax.random.permutation(shard_key, BYTE_DEV - 1)
        cut = (order < count - 1).astype(jnp.int32)
        return jnp.concatenate([jnp.zeros((1,), jnp.int32), jnp.cumsum(cut).astype(jnp.int32)])
    return jax.vmap(one_shard)(shard_keys, counts).reshape(-1).astype(jnp.int32)


def draw_byte_states(key, part):
    values = jax.random.normal(key, (BYTES, DL), jnp.float32)
    return jnp.clip(values, -12.0, 12.0).astype(jnp.bfloat16)


def draw_w_qkv(key, part):
    values = jax.random.normal(key, (3, DL, HEADS * HD), jnp.float32) * DL ** (-0.5)
    return jnp.clip(values, -0.25, 0.25).astype(jnp.bfloat16)


def shard_levels(own_key, extent, cuts, least, top_value):
    level, own = 1.0, jax.random.fold_in(own_key, 6)
    for dim, parts in cuts:
        steps = jnp.exp(jax.random.uniform(jax.random.fold_in(own, dim), (parts,), jnp.float32, least / len(cuts), top_value / len(cuts)))
        level = level * jnp.repeat(steps, extent[dim] // parts).reshape([-1 if axis == dim else 1 for axis in range(len(extent))])
    return level


def scatter_about(own_key, extent, deviation, most, cuts=(), held_as=jnp.bfloat16):
    loudness = shard_levels(own_key, extent, cuts, -0.22, 0.18) if cuts else 1.0
    entries = jax.random.normal(own_key, extent, jnp.float32) * deviation * loudness
    return jnp.minimum(jnp.maximum(entries, -most), most).astype(held_as)


def setup_inputs(seed: int = 0) -> dict:
    key_list = jax.random.split(jax.random.key(seed), 7)
    return {
        "byte_states": draw_byte_states(jax.random.fold_in(key_list[6], 71), 0),
        "patch_of_byte": draw_patch_of_byte(jax.random.fold_in(key_list[6], 71), 0),
        "patch_first": draw_patch_first(jax.random.fold_in(key_list[6], 71), 0),
        "moved": draw_moved(jax.random.fold_in(key_list[6], 71), 0),
        "w_qkv": draw_w_qkv(jax.random.fold_in(key_list[6], 71), 0),
        "d_attn": scatter_about(key_list[5], (KEYS, HEADS * HD), 1.0, 6.0, ((0, 16), (1, 2))),
    }


def reference(byte_states, patch_of_byte, patch_first, moved, w_qkv, d_attn):
    shard = jnp.arange(BYTES, dtype=jnp.int32) // BYTE_DEV
    gid = (patch_first[shard] + patch_of_byte).astype(jnp.int32)
    sums = jax.ops.segment_sum(byte_states.astype(jnp.float32), gid, num_segments=KEYS)
    lengths = jax.ops.segment_sum(jnp.ones((BYTES,), jnp.float32), gid, num_segments=KEYS)
    pooled_global = (sums / lengths[:, None]).astype(jnp.bfloat16)

    place = jnp.arange(KEYS, dtype=jnp.int32)
    ends = jnp.concatenate([patch_first[1:], jnp.full((1,), KEYS, jnp.int32)]).astype(jnp.int32)
    counts = (ends - patch_first).astype(jnp.int32)
    lower_moves = moved[0]
    upper_moves = moved[1]
    below_high = jnp.concatenate([jnp.zeros((1,), jnp.int32), upper_moves[:-1]]).astype(jnp.int32)
    home = (jnp.sum((place[:, None] >= patch_first[None, :]).astype(jnp.int32), axis=1) - 1).astype(jnp.int32)
    local = (place - patch_first[home]).astype(jnp.int32)
    low_here = lower_moves[home]
    high_here = upper_moves[home]
    count_here = counts[home]
    goes_low = local < low_here
    goes_high = local >= count_here - high_here
    owner = jnp.where(goes_low, home - 1, jnp.where(goes_high, home + 1, home))
    rank = jnp.where(goes_low, P_DEV - low_here + local,
                     jnp.where(goes_high, local - (count_here - high_here), below_high[home] + local - low_here))
    slot = (owner * P_DEV + rank).astype(jnp.int32)
    order = jnp.zeros((KEYS,), jnp.int32).at[slot].set(place)

    pooled = pooled_global[order]
    query = jnp.dot(pooled, w_qkv[0], preferred_element_type=jnp.float32).astype(jnp.bfloat16)
    keyed = jnp.dot(pooled, w_qkv[1], preferred_element_type=jnp.float32).astype(jnp.bfloat16)
    valued = jnp.dot(pooled, w_qkv[2], preferred_element_type=jnp.float32).astype(jnp.bfloat16)
    scale = HD ** -0.5
    causal = order[:, None] >= order[None, :]

    def heads_first(x):
        return jnp.transpose(x.reshape(KEYS, HEADS, HD), (1, 0, 2))

    def per_head(items):
        q_head, k_head, v_head, g_head = items
        score = jnp.dot(q_head, k_head.T, preferred_element_type=jnp.float32) * scale
        masked = jnp.where(causal, score, -jnp.inf)
        top = jnp.max(masked, axis=1, keepdims=True)
        lse = top + jnp.log(jnp.sum(jnp.exp(masked - top), axis=1, keepdims=True))
        prob = jnp.exp(jnp.where(causal, score - lse, -jnp.inf))
        probs = prob.astype(jnp.bfloat16)
        output = jnp.dot(probs, v_head, preferred_element_type=jnp.float32).astype(jnp.bfloat16)
        delta = jnp.sum(g_head.astype(jnp.float32) * output.astype(jnp.float32), axis=1, keepdims=True)
        dprob = jnp.dot(g_head, v_head.T, preferred_element_type=jnp.float32)
        dscore = (prob * (dprob - delta)).astype(jnp.bfloat16)
        d_query = (jnp.dot(dscore, k_head, preferred_element_type=jnp.float32) * scale).astype(jnp.bfloat16)
        d_key = (jnp.dot(dscore.T, q_head, preferred_element_type=jnp.float32) * scale).astype(jnp.bfloat16)
        d_value = jnp.dot(probs.T, g_head, preferred_element_type=jnp.float32).astype(jnp.bfloat16)
        return output, d_query, d_key, d_value

    results = lax.map(per_head, (heads_first(query), heads_first(keyed), heads_first(valued), heads_first(d_attn)))

    def rows_first(x):
        return jnp.transpose(x, (1, 0, 2)).reshape(KEYS, HEADS * HD)

    attn_out = rows_first(results[0])
    d_query, d_key, d_value = rows_first(results[1]), rows_first(results[2]), rows_first(results[3])
    d_pooled = jnp.dot(d_query, w_qkv[0].T, preferred_element_type=jnp.float32)
    d_pooled = d_pooled + jnp.dot(d_key, w_qkv[1].T, preferred_element_type=jnp.float32)
    d_pooled = d_pooled + jnp.dot(d_value, w_qkv[2].T, preferred_element_type=jnp.float32)
    d_pooled = d_pooled.astype(jnp.bfloat16)
    byte_slot = slot[gid]
    byte_grad = (d_pooled[byte_slot].astype(jnp.float32) / lengths[gid][:, None]).astype(jnp.bfloat16)
    return attn_out, byte_grad
```

```python
import functools

import jax
import jax.numpy as jnp
from jax import lax
from jax.experimental import pallas as pl
from jax.experimental.pallas import tpu as pltpu
from jax.sharding import PartitionSpec as P

HD = 128
MESH = pl.DeviceIdType.MESH
VM = pl.BlockSpec(memory_space=pltpu.VMEM)


def remote(src, dst, send, recv, device):
    return pltpu.make_async_remote_copy(
        src_ref=src, dst_ref=dst, send_sem=send, recv_sem=recv, device_id=device, device_id_type=MESH
    )


def neighbours_kernel(n, blk_ref, out_ref, send_sem, recv_sem):
    me = lax.axis_index("ctx")
    left, right = lax.rem(me + n - 1, n), lax.rem(me + 1, n)
    barrier = pltpu.get_barrier_semaphore()
    for peer in (left, right):
        pl.semaphore_signal(barrier, inc=1, device_id={"ctx": peer}, device_id_type=MESH)
    pl.semaphore_wait(barrier, 2)
    copies = [
        remote(blk_ref.at[i], out_ref.at[i], send_sem.at[i], recv_sem.at[i], {"ctx": peer})
        for i, peer in enumerate((left, right))
    ]
    for copy in copies:
        copy.start()
    for copy in copies:
        copy.wait()


def neighbours(blk, n):
    return pl.pallas_call(
        functools.partial(neighbours_kernel, n),
        out_shape=jax.ShapeDtypeStruct(blk.shape, blk.dtype),
        in_specs=[VM],
        out_specs=VM,
        scratch_shapes=[pltpu.SemaphoreType.DMA((2,)), pltpu.SemaphoreType.DMA((2,))],
        compiler_params=pltpu.CompilerParams(collective_id=0, has_side_effects=True),
        name="neighbours",
    )(blk)


def attend_kernel(
    n, heads, rows, block,
    q_ref, k_ref, v_ref, g_ref, qid_ref, kid_ref,
    o_out, dq_out, dk_out, dv_out,
    qb, gb, kb, vb, ob, dqb, dkb, dvb, dka, dva,
    send_kv, recv_kv, send_qg, recv_qg, send_dkv, recv_dkv, send_odq, recv_odq, local_sem,
):
    groups = n // heads
    total = n * rows
    scale = HD ** (-0.5)
    me = lax.axis_index("ctx")
    my_head, my_group = me // groups, lax.rem(me, groups)

    def cols(head):
        return pl.ds(pl.multiple_of(head * HD, HD), HD)

    barrier = pltpu.get_barrier_semaphore()

    def greet(i, carry):
        peer = lax.rem(me + i, n)
        pl.semaphore_signal(barrier, inc=1, device_id={"ctx": peer}, device_id_type=MESH)
        return carry

    lax.fori_loop(1, n, greet, 0)
    pl.semaphore_wait(barrier, n - 1)

    def mate(i):
        return lax.rem(my_head + i, heads)

    def to_peer(i):
        peer = lax.rem(me + i, n)
        c = cols(peer // groups)
        return (
            remote(k_ref.at[:, c], kb.at[me], send_kv.at[0, i], recv_kv.at[0, i], {"ctx": peer}),
            remote(v_ref.at[:, c], vb.at[me], send_kv.at[1, i], recv_kv.at[1, i], {"ctx": peer}),
        )

    def to_mate(i):
        head = mate(i)
        peer = head * groups + my_group
        c = cols(head)
        return (
            remote(g_ref.at[:, c], gb.at[my_head], send_qg.at[0, i], recv_qg.at[0, i], {"ctx": peer}),
            remote(q_ref.at[:, c], qb.at[my_head], send_qg.at[1, i], recv_qg.at[1, i], {"ctx": peer}),
        )

    def back_peer(i):
        peer = lax.rem(me + i, n)
        c = cols(my_head)
        return (
            remote(dkb.at[peer], dk_out.at[my_group, :, c], send_dkv.at[0, i], recv_dkv.at[0, i], {"ctx": peer}),
            remote(dvb.at[peer], dv_out.at[my_group, :, c], send_dkv.at[1, i], recv_dkv.at[1, i], {"ctx": peer}),
        )

    def back_mate(i):
        head = mate(i)
        peer = head * groups + my_group
        c = cols(my_head)
        return (
            remote(ob.at[head], o_out.at[:, c], send_odq.at[0, i], recv_odq.at[0, i], {"ctx": peer}),
            remote(dqb.at[head], dq_out.at[:, c], send_odq.at[1, i], recv_odq.at[1, i], {"ctx": peer}),
        )

    def start_all(make):
        def body(i, carry):
            for copy in make(i):
                copy.start()
            return carry
        return body

    def wait_all(make):
        def body(i, carry):
            for copy in make(i):
                copy.wait()
            return carry
        return body

    lax.fori_loop(1, n, start_all(to_peer), 0)
    lax.fori_loop(1, heads, start_all(to_mate), 0)
    mine = cols(my_head)
    own = [
        pltpu.make_async_copy(src.at[:, mine], dst, local_sem.at[i])
        for i, (src, dst) in enumerate((
            (k_ref, kb.at[me]), (v_ref, vb.at[me]), (g_ref, gb.at[my_head]), (q_ref, qb.at[my_head])
        ))
    ]
    for copy in own:
        copy.start()
    dka[...] = jnp.zeros_like(dka)
    dva[...] = jnp.zeros_like(dva)
    for copy in own:
        copy.wait()
    lax.fori_loop(1, heads, wait_all(to_mate), 0)
    lax.fori_loop(1, n, wait_all(to_peer), 0)

    over_last = (((1,), (1,)), ((), ()))
    over_first = (((0,), (0,)), ((), ()))

    def step(b, carry):
        first = b * block
        q = qb[pl.ds(first, block)].reshape(block * rows, HD)
        g = gb[pl.ds(first, block)].reshape(block * rows, HD)
        k = kb[...].reshape(total, HD)
        v = vb[...].reshape(total, HD)
        qid = qid_ref[pl.ds(pl.multiple_of(first * rows, rows), block * rows), :]
        allowed = qid >= kid_ref[...]
        score = lax.dot_general(q, k, over_last, preferred_element_type=jnp.float32) * scale
        score = jnp.where(allowed, score, -jnp.inf)
        top = jnp.max(score, axis=1, keepdims=True)
        e = jnp.exp(score - top)
        prob = e * (1.0 / jnp.sum(e, axis=1, keepdims=True))
        probs = prob.astype(jnp.bfloat16)
        out = jnp.dot(probs, v, preferred_element_type=jnp.float32).astype(jnp.bfloat16)
        delta = jnp.sum(g.astype(jnp.float32) * out.astype(jnp.float32), axis=1, keepdims=True)
        dprob = lax.dot_general(g, v, over_last, preferred_element_type=jnp.float32)
        dscore = (prob * (dprob - delta)).astype(jnp.bfloat16)
        dq = (jnp.dot(dscore, k, preferred_element_type=jnp.float32) * scale).astype(jnp.bfloat16)
        ob[pl.ds(first, block)] = out.reshape(block, rows, HD)
        dqb[pl.ds(first, block)] = dq.reshape(block, rows, HD)
        dka[...] += lax.dot_general(dscore, q, over_first, preferred_element_type=jnp.float32)
        dva[...] += lax.dot_general(probs, g, over_first, preferred_element_type=jnp.float32)
        return carry

    lax.fori_loop(0, heads // block, step, 0)
    dkb[...] = (dka[...] * scale).astype(jnp.bfloat16).reshape(n, rows, HD)
    dvb[...] = dva[...].astype(jnp.bfloat16).reshape(n, rows, HD)

    lax.fori_loop(1, n, start_all(back_peer), 0)
    lax.fori_loop(1, heads, start_all(back_mate), 0)
    own = [
        pltpu.make_async_copy(src, dst, local_sem.at[i])
        for i, (src, dst) in enumerate((
            (dkb.at[me], dk_out.at[my_group, :, mine]), (dvb.at[me], dv_out.at[my_group, :, mine]),
            (ob.at[my_head], o_out.at[:, mine]), (dqb.at[my_head], dq_out.at[:, mine]),
        ))
    ]
    for copy in own:
        copy.start()
    for copy in own:
        copy.wait()
    lax.fori_loop(1, heads, wait_all(back_mate), 0)
    lax.fori_loop(1, n, wait_all(back_peer), 0)


def attend(query, keyed, valued, grad, qid, kid, n):
    rows, feats = query.shape
    heads = feats // HD
    groups = n // heads
    total = n * rows
    block = 2 if heads % 2 == 0 else 1
    bf = jnp.bfloat16
    dma = pltpu.SemaphoreType.DMA
    return pl.pallas_call(
        functools.partial(attend_kernel, n, heads, rows, block),
        out_shape=[
            jax.ShapeDtypeStruct((rows, feats), bf),
            jax.ShapeDtypeStruct((rows, feats), bf),
            jax.ShapeDtypeStruct((groups, rows, feats), bf),
            jax.ShapeDtypeStruct((groups, rows, feats), bf),
        ],
        in_specs=[VM] * 6,
        out_specs=[VM] * 4,
        scratch_shapes=[
            pltpu.VMEM((heads, rows, HD), bf), pltpu.VMEM((heads, rows, HD), bf),
            pltpu.VMEM((n, rows, HD), bf), pltpu.VMEM((n, rows, HD), bf),
            pltpu.VMEM((heads, rows, HD), bf), pltpu.VMEM((heads, rows, HD), bf),
            pltpu.VMEM((n, rows, HD), bf), pltpu.VMEM((n, rows, HD), bf),
            pltpu.VMEM((total, HD), jnp.float32), pltpu.VMEM((total, HD), jnp.float32),
            dma((2, n)), dma((2, n)), dma((2, heads)), dma((2, heads)),
            dma((2, n)), dma((2, n)), dma((2, heads)), dma((2, heads)), dma((4,)),
        ],
        compiler_params=pltpu.CompilerParams(
            collective_id=1, has_side_effects=True, vmem_limit_bytes=48 << 20
        ),
        name="attend",
    )(query, keyed, valued, grad, qid, kid)


def returning_kernel(n, tp, half, rows, part_ref, own_ref, lo_ref, hi_ref, send_sem, recv_sem, local_sem):
    me, mt = lax.axis_index("ctx"), lax.axis_index("tp")
    left, right = lax.rem(me + n - 1, n), lax.rem(me + 1, n)
    peers = [(me, lax.rem(mt + i, tp)) for i in range(1, tp)]
    peers += [(side, lax.rem(mt + i, tp)) for side in (left, right) for i in range(tp)]
    barrier = pltpu.get_barrier_semaphore()
    for peer in peers:
        pl.semaphore_signal(barrier, inc=1, device_id=peer, device_id_type=MESH)
    pl.semaphore_wait(barrier, len(peers))
    first, last = pl.ds(0, half), pl.ds(rows - half, half)
    copies = []
    for at, (c, t) in enumerate(peers):
        if at < tp - 1:
            src, dst = part_ref.at[t], own_ref.at[mt]
        elif at < 2 * tp - 1:
            src, dst = part_ref.at[t, first], hi_ref.at[mt]
        else:
            src, dst = part_ref.at[t, last], lo_ref.at[mt]
        copies.append(remote(src, dst, send_sem.at[at], recv_sem.at[at], (c, t)))
    for copy in copies:
        copy.start()
    mine = pltpu.make_async_copy(part_ref.at[mt], own_ref.at[mt], local_sem)
    mine.start()
    mine.wait()
    for copy in copies:
        copy.wait()


def returning(part, n):
    tp, rows, width = part.shape
    half = rows // 2
    dma = pltpu.SemaphoreType.DMA
    return pl.pallas_call(
        functools.partial(returning_kernel, n, tp, half, rows),
        out_shape=[
            jax.ShapeDtypeStruct((tp, rows, width), part.dtype),
            jax.ShapeDtypeStruct((tp, half, width), part.dtype),
            jax.ShapeDtypeStruct((tp, half, width), part.dtype),
        ],
        in_specs=[VM],
        out_specs=[VM] * 3,
        scratch_shapes=[dma((3 * tp - 1,)), dma((3 * tp - 1,)), dma],
        compiler_params=pltpu.CompilerParams(collective_id=2, has_side_effects=True),
        name="returning",
    )(part)


def shards(byte_states, patch_of_byte, patch_first, moved, w_qkv, d_attn):
    me = lax.axis_index("ctx")
    n = lax.axis_size("ctx")
    tp = lax.axis_size("tp")
    rows, feats = d_attn.shape
    half = rows // 2
    heads = feats // HD
    groups = n // heads
    total = rows * n
    model = byte_states.shape[1]
    zero_one = jnp.zeros((1,), jnp.int32)
    ends = jnp.concatenate([patch_first[1:], jnp.full((1,), total, jnp.int32)])
    counts = ends - patch_first
    lower, upper = moved[0], moved[1]
    below = jnp.concatenate([zero_one, upper[:-1]])
    above = jnp.concatenate([lower[1:], zero_one])
    ranks = jnp.arange(rows, dtype=jnp.int32)[None, :]
    ids = jnp.where(
        ranks < below[:, None],
        patch_first[:, None] - below[:, None] + ranks,
        jnp.where(
            ranks >= (rows - above)[:, None],
            ends[:, None] + ranks - (rows - above)[:, None],
            patch_first[:, None] + lower[:, None] + ranks - below[:, None],
        ),
    )
    kid = ids.reshape(1, total)
    qid = lax.dynamic_index_in_dim(
        ids.reshape(heads, groups, rows), lax.rem(me, groups), 1, keepdims=False
    ).reshape(heads * rows, 1)

    def own(values):
        return lax.dynamic_index_in_dim(values, me, 0, keepdims=False)

    my_count, my_low, my_high = own(counts), own(lower), own(upper)
    my_below, my_above = own(below), own(above)
    rank = jnp.arange(rows, dtype=jnp.int32)
    part_rank = jnp.arange(half, dtype=jnp.int32)
    own_local = jnp.where(
        (rank >= my_below) & (rank < rows - my_above), my_low + rank - my_below, -1
    )
    down = part_rank - half + my_low
    up = jnp.where(part_rank < my_high, my_count - my_high + part_rank, -1)
    wanted = jnp.concatenate([down, up, own_local])
    member = patch_of_byte[None, :] == wanted[:, None]
    lengths = jnp.sum(member.astype(jnp.float32), axis=1)
    pooled_all = (
        jnp.dot(member.astype(jnp.bfloat16), byte_states, preferred_element_type=jnp.float32)
        / jnp.maximum(lengths, 1.0)[:, None]
    ).astype(jnp.bfloat16)
    came = neighbours(pooled_all[: 2 * half].reshape(2, half, model), n)
    pooled = pooled_all[2 * half :] + jnp.concatenate([came[1], came[0]], axis=0)
    query = jnp.dot(pooled, w_qkv[0], preferred_element_type=jnp.float32).astype(jnp.bfloat16)
    keyed = jnp.dot(pooled, w_qkv[1], preferred_element_type=jnp.float32).astype(jnp.bfloat16)
    valued = jnp.dot(pooled, w_qkv[2], preferred_element_type=jnp.float32).astype(jnp.bfloat16)
    attn_out, d_query, d_key, d_value = attend(query, keyed, valued, d_attn, qid, kid, n)
    d_key = jnp.sum(d_key.astype(jnp.float32), axis=0).astype(jnp.bfloat16)
    d_value = jnp.sum(d_value.astype(jnp.float32), axis=0).astype(jnp.bfloat16)
    contract = (((1,), (1,)), ((), ()))
    partial = lax.dot_general(d_query, w_qkv[0], contract, preferred_element_type=jnp.float32)
    partial += lax.dot_general(d_key, w_qkv[1], contract, preferred_element_type=jnp.float32)
    partial += lax.dot_general(d_value, w_qkv[2], contract, preferred_element_type=jnp.float32)
    width = model // tp
    part = jnp.transpose(partial.astype(jnp.bfloat16).reshape(rows, tp, width), (1, 0, 2))
    own_part, lo_part, hi_part = returning(part, n)
    stacked = jnp.concatenate([lo_part, own_part, hi_part], axis=1)
    returned = jnp.sum(stacked.astype(jnp.float32), axis=0).astype(jnp.bfloat16)
    target = jnp.where(
        patch_of_byte < my_low,
        half - my_low + patch_of_byte,
        jnp.where(
            patch_of_byte >= my_count - my_high,
            half + rows + patch_of_byte - (my_count - my_high),
            half + my_below + patch_of_byte - my_low,
        ),
    )
    chooser = (target[:, None] == jnp.arange(2 * rows, dtype=jnp.int32)[None, :]).astype(jnp.bfloat16)
    spread = jnp.dot(chooser, returned, preferred_element_type=jnp.float32)
    same = (patch_of_byte[:, None] == patch_of_byte[None, :]).astype(jnp.float32)
    byte_lengths = jnp.sum(same, axis=1)
    byte_grad = (spread / byte_lengths[:, None]).astype(jnp.bfloat16)
    return attn_out, byte_grad


def solution(mesh):
    placed = (P("ctx", None), P("ctx"), P(), P(), P(None, None, "tp"), P("ctx", "tp"))
    return jax.shard_map(
        shards,
        mesh=mesh,
        in_specs=placed,
        out_specs=(P("ctx", "tp"), P("ctx", "tp")),
        check_vma=False,
    )
```

```python
import functools

import jax
import jax.numpy as jnp
from jax import lax
from jax.experimental import pallas as pl
from jax.experimental.pallas import tpu as pltpu
from jax.sharding import PartitionSpec as P

HD = 128
MESH = pl.DeviceIdType.MESH
VM = pl.BlockSpec(memory_space=pltpu.VMEM)


def remote(src, dst, send, recv, device):
    return pltpu.make_async_remote_copy(
        src_ref=src, dst_ref=dst, send_sem=send, recv_sem=recv, device_id=device, device_id_type=MESH
    )


def whole_kernel(
    n, tp, heads, rows, block,
    bytes_ref, pob_ref, first_ref, moved_ref, w_ref, d_ref,
    attn_ref, grad_ref,
    blk, came, pooled, wbuf, own3, qb, gb, kb, vb, ob, dqb, dkb, dvb, dka, dva,
    o_in, dq_in, dk_in, dv_in, part, own_part, lo_part, hi_part,
    w_sem, send_nb, recv_nb, send_kv, recv_kv, send_qg, recv_qg,
    send_dkv, recv_dkv, send_odq, recv_odq, send_rt, recv_rt, local_sem,
):
    groups = n // heads
    total = n * rows
    half = rows // 2
    scale = HD ** (-0.5)
    bf, f32 = jnp.bfloat16, jnp.float32
    me, mt = lax.axis_index("ctx"), lax.axis_index("tp")
    my_head, my_group = me // groups, lax.rem(me, groups)
    left, right = lax.rem(me + n - 1, n), lax.rem(me + 1, n)
    width = part.shape[2]

    def cols(head):
        return pl.ds(pl.multiple_of(head * HD, HD), HD)

    barrier = pltpu.get_barrier_semaphore()

    def greet(i, carry):
        peer = lax.rem(me + i, n)
        pl.semaphore_signal(barrier, inc=1, device_id=(peer, mt), device_id_type=MESH)
        return carry

    lax.fori_loop(1, n, greet, 0)
    for c in (me, left, right):
        for i in range(1, tp):
            pl.semaphore_signal(
                barrier, inc=1, device_id=(c, lax.rem(mt + i, tp)), device_id_type=MESH
            )
    loads = [pltpu.make_async_copy(w_ref.at[j], wbuf.at[j], w_sem.at[j]) for j in range(3)]
    for j in (1, 2, 0):
        loads[j].start()

    def plan(c):
        below = moved_ref[1, lax.rem(c + n - 1, n)]
        above = moved_ref[0, lax.rem(c + 1, n)]
        start = first_ref[c]
        end = jnp.where(c == n - 1, total, first_ref[lax.rem(c + 1, n)])
        return start, end, below, above, moved_ref[0, c], moved_ref[1, c]

    def numbers(c, rank):
        start, end, below, above, low, high = plan(c)
        return jnp.where(
            rank < below,
            start - below + rank,
            jnp.where(rank >= rows - above, end + rank - (rows - above), start + low + rank - below),
        )

    start, end, below, above, low, high = plan(me)
    count = end - start
    rank = lax.broadcasted_iota(jnp.int32, (2 * rows, 1), 0)
    own_rank = rank - 2 * half
    own_local = jnp.where((own_rank >= below) & (own_rank < rows - above), low + own_rank - below, -1)
    up = jnp.where(rank - half < high, count - high + rank - half, -1)
    wanted = jnp.where(rank < half, rank - half + low, jnp.where(rank < 2 * half, up, own_local))
    pob = pob_ref[...]
    member = (pob == wanted).astype(f32)
    lengths = jnp.maximum(jnp.sum(member, axis=1, keepdims=True), 1.0)
    means = (
        jnp.dot(member.astype(bf), bytes_ref[...], preferred_element_type=f32) / lengths
    ).astype(bf)
    blk[0] = means[:half]
    blk[1] = means[half : 2 * half]
    pl.semaphore_wait(barrier, n - 1 + 3 * (tp - 1))
    near = [
        remote(blk.at[i], came.at[i], send_nb.at[i], recv_nb.at[i], (peer, mt))
        for i, peer in enumerate((left, right))
    ]
    for copy in near:
        copy.start()

    def over_peers(make, wait=False):
        def body(i, carry):
            copy = make(i)
            if wait:
                copy.wait()
            else:
                copy.start()
            return carry

        lax.fori_loop(1, n, body, 0)

    def over_mates(make, wait=False):
        def body(i, carry):
            copy = make(i)
            if wait:
                copy.wait()
            else:
                copy.start()
            return carry

        lax.fori_loop(1, heads, body, 0)

    def to_peer(a, ref, out):
        def make(i):
            peer = lax.rem(me + i, n)
            return remote(
                ref.at[:, cols(peer // groups)], out.at[me], send_kv.at[a, i], recv_kv.at[a, i], (peer, mt)
            )

        return make

    def to_mate(a, ref, out):
        def make(i):
            head = lax.rem(my_head + i, heads)
            return remote(
                ref.at[:, cols(head)], out.at[my_head], send_qg.at[a, i], recv_qg.at[a, i],
                (head * groups + my_group, mt),
            )

        return make

    def back_peer(a, ref, out):
        def make(i):
            peer = lax.rem(me + i, n)
            return remote(
                ref.at[peer], out.at[my_group, :, cols(my_head)], send_dkv.at[a, i], recv_dkv.at[a, i],
                (peer, mt),
            )

        return make

    def back_mate(a, ref, out):
        def make(i):
            head = lax.rem(my_head + i, heads)
            return remote(
                ref.at[head], out.at[:, cols(my_head)], send_odq.at[a, i], recv_odq.at[a, i],
                (head * groups + my_group, mt),
            )

        return make

    mine = cols(my_head)
    send_g = to_mate(0, d_ref, gb)
    send_q = to_mate(1, own3.at[0], qb)
    send_k = to_peer(0, own3.at[1], kb)
    send_v = to_peer(1, own3.at[2], vb)
    over_mates(send_g)
    for copy in near:
        copy.wait()
    pooled[pl.ds(0, half)] = means[2 * half : 3 * half] + came[1]
    pooled[pl.ds(half, half)] = means[3 * half :] + came[0]
    for j, send in ((1, lambda: over_peers(send_k)), (2, lambda: over_peers(send_v)), (0, lambda: over_mates(send_q))):
        loads[j].wait()
        own3[j] = jnp.dot(pooled[...], wbuf[j], preferred_element_type=f32).astype(bf)
        send()
    own = [
        pltpu.make_async_copy(src, dst, local_sem.at[i])
        for i, (src, dst) in enumerate((
            (own3.at[1, :, mine], kb.at[me]), (own3.at[2, :, mine], vb.at[me]),
            (d_ref.at[:, mine], gb.at[my_head]), (own3.at[0, :, mine], qb.at[my_head]),
        ))
    ]
    for copy in own:
        copy.start()
    dka[...] = jnp.zeros_like(dka)
    dva[...] = jnp.zeros_like(dva)
    lane = lax.broadcasted_iota(jnp.int32, (1, total), 1)

    def number_keys(c, ids):
        return jnp.where((lane >= c * rows) & (lane < (c + 1) * rows), numbers(c, lane - c * rows), ids)

    kid = lax.fori_loop(0, n, number_keys, jnp.zeros((1, total), jnp.int32))
    for copy in own:
        copy.wait()
    over_mates(send_g, True)
    over_peers(send_k, True)
    over_peers(send_v, True)
    over_mates(send_q, True)

    over_last = (((1,), (1,)), ((), ()))
    over_first = (((0,), (0,)), ((), ()))
    back_o, back_q = back_mate(0, ob, o_in), back_mate(1, dqb, dq_in)
    row = lax.broadcasted_iota(jnp.int32, (rows, 1), 0)
    step_keys = 128 // rows if rows < 128 else 1
    for b in range(heads // block):
        lo = b * block
        reach = min(n, (lo + block) * groups + 1)
        reach = min(n, -(-reach // step_keys) * step_keys)
        keys = reach * rows
        q = qb[pl.ds(lo, block)].reshape(block * rows, HD)
        g = gb[pl.ds(lo, block)].reshape(block * rows, HD)
        k = kb[pl.ds(0, reach)].reshape(keys, HD)
        v = vb[pl.ds(0, reach)].reshape(keys, HD)
        qid = jnp.concatenate([numbers((lo + j) * groups + my_group, row) for j in range(block)], axis=0)
        allowed = qid >= kid[:, :keys]
        score = lax.dot_general(q, k, over_last, preferred_element_type=f32) * scale
        score = jnp.where(allowed, score, -jnp.inf)
        top = jnp.max(score, axis=1, keepdims=True)
        e = jnp.exp(score - top)
        prob = e * (1.0 / jnp.sum(e, axis=1, keepdims=True))
        probs = prob.astype(bf)
        out = jnp.dot(probs, v, preferred_element_type=f32).astype(bf)
        delta = jnp.sum(g.astype(f32) * out.astype(f32), axis=1, keepdims=True)
        dprob = lax.dot_general(g, v, over_last, preferred_element_type=f32)
        dscore = (prob * (dprob - delta)).astype(bf)
        dq = (jnp.dot(dscore, k, preferred_element_type=f32) * scale).astype(bf)
        ob[pl.ds(lo, block)] = out.reshape(block, rows, HD)
        dqb[pl.ds(lo, block)] = dq.reshape(block, rows, HD)
        dka[pl.ds(0, keys)] += lax.dot_general(dscore, q, over_first, preferred_element_type=f32)
        dva[pl.ds(0, keys)] += lax.dot_general(probs, g, over_first, preferred_element_type=f32)
        for j in range(block):
            i = lax.rem(lo + j - my_head + heads, heads)

            @pl.when(i != 0)
            def _():
                back_o(i).start()
                back_q(i).start()

    send_dk, send_dv = back_peer(0, dkb, dk_in), back_peer(1, dvb, dv_in)
    dvb[...] = dva[...].astype(bf).reshape(n, rows, HD)
    over_peers(send_dv)
    dkb[...] = (dka[...] * scale).astype(bf).reshape(n, rows, HD)
    over_peers(send_dk)
    own = [
        pltpu.make_async_copy(src, dst, local_sem.at[i])
        for i, (src, dst) in enumerate((
            (dkb.at[me], dk_in.at[my_group, :, mine]), (dvb.at[me], dv_in.at[my_group, :, mine]),
            (ob.at[my_head], o_in.at[:, mine]), (dqb.at[my_head], dq_in.at[:, mine]),
        ))
    ]
    for copy in own:
        copy.start()
    for copy in own:
        copy.wait()
    over_mates(back_o, True)
    attn_ref[...] = o_in[...]
    over_mates(back_q, True)
    partial = lax.dot_general(dq_in[...], wbuf[0], over_last, preferred_element_type=f32)
    for send, held, j in ((send_dv, dv_in, 2), (send_dk, dk_in, 1)):
        over_peers(send, True)
        summed = held[0].astype(f32)
        for i in range(1, groups):
            summed = summed + held[i].astype(f32)
        partial += lax.dot_general(summed.astype(bf), wbuf[j], over_last, preferred_element_type=f32)
    for t in range(tp):
        part[t] = partial[:, t * width : (t + 1) * width].astype(bf)
    edge_lo, edge_hi = pl.ds(0, half), pl.ds(rows - half, half)
    copies = []
    for i in range(1, tp):
        t = lax.rem(mt + i, tp)
        copies.append((part.at[t], own_part.at[mt], (me, t)))
    for i in range(tp):
        t = lax.rem(mt + i, tp)
        copies.append((part.at[t, edge_lo], hi_part.at[mt], (left, t)))
        copies.append((part.at[t, edge_hi], lo_part.at[mt], (right, t)))
    copies = [
        remote(src, dst, send_rt.at[i], recv_rt.at[i], peer) for i, (src, dst, peer) in enumerate(copies)
    ]
    for copy in copies:
        copy.start()
    kept = pltpu.make_async_copy(part.at[mt], own_part.at[mt], local_sem.at[0])
    kept.start()
    target = jnp.where(
        pob < low,
        half - low + pob,
        jnp.where(pob >= count - high, half + rows + pob - (count - high), half + below + pob - low),
    )
    chooser = (target == lax.broadcasted_iota(jnp.int32, (2 * rows, 1), 0)).astype(f32)
    sizes = jnp.maximum(jnp.sum(chooser, axis=1, keepdims=True), 1.0)
    kept.wait()
    for copy in copies:
        copy.wait()

    def over_tp(ref):
        value = ref[0].astype(f32)
        for i in range(1, tp):
            value = value + ref[i].astype(f32)
        return value

    returned = jnp.concatenate([over_tp(lo_part), over_tp(own_part), over_tp(hi_part)], axis=0)
    shares = (returned.astype(bf).astype(f32) / sizes).astype(bf)
    grad_ref[...] = lax.dot_general(
        chooser.astype(bf), shares, over_first, preferred_element_type=f32
    ).astype(bf)


def shards(byte_states, patch_of_byte, patch_first, moved, w_qkv, d_attn):
    n, tp = lax.axis_size("ctx"), lax.axis_size("tp")
    rows, feats = d_attn.shape
    size, model = byte_states.shape
    heads = feats // HD
    groups = n // heads
    total = n * rows
    half = rows // 2
    width = model // tp
    block = 2 if heads % 2 == 0 else 1
    bf, f32 = jnp.bfloat16, jnp.float32
    dma = pltpu.SemaphoreType.DMA
    smem = pl.BlockSpec(memory_space=pltpu.SMEM)
    return tuple(pl.pallas_call(
        functools.partial(whole_kernel, n, tp, heads, rows, block),
        out_shape=[
            jax.ShapeDtypeStruct((rows, feats), bf),
            jax.ShapeDtypeStruct((size, width), bf),
        ],
        in_specs=[VM, VM, smem, smem, pl.BlockSpec(memory_space=pl.ANY), VM],
        out_specs=[VM] * 2,
        scratch_shapes=[
            pltpu.VMEM((2, half, model), bf), pltpu.VMEM((2, half, model), bf),
            pltpu.VMEM((rows, model), bf), pltpu.VMEM(w_qkv.shape, bf), pltpu.VMEM((3, rows, feats), bf),
            pltpu.VMEM((heads, rows, HD), bf), pltpu.VMEM((heads, rows, HD), bf),
            pltpu.VMEM((n, rows, HD), bf), pltpu.VMEM((n, rows, HD), bf),
            pltpu.VMEM((heads, rows, HD), bf), pltpu.VMEM((heads, rows, HD), bf),
            pltpu.VMEM((n, rows, HD), bf), pltpu.VMEM((n, rows, HD), bf),
            pltpu.VMEM((total, HD), f32), pltpu.VMEM((total, HD), f32),
            pltpu.VMEM((rows, feats), bf), pltpu.VMEM((rows, feats), bf),
            pltpu.VMEM((groups, rows, feats), bf), pltpu.VMEM((groups, rows, feats), bf),
            pltpu.VMEM((tp, rows, width), bf), pltpu.VMEM((tp, rows, width), bf),
            pltpu.VMEM((tp, half, width), bf), pltpu.VMEM((tp, half, width), bf),
            dma((3,)), dma((2,)), dma((2,)), dma((2, n)), dma((2, n)), dma((2, heads)), dma((2, heads)),
            dma((2, n)), dma((2, n)), dma((2, heads)), dma((2, heads)),
            dma((3 * tp - 1,)), dma((3 * tp - 1,)), dma((4,)),
        ],
        compiler_params=pltpu.CompilerParams(
            collective_id=0, has_side_effects=True, vmem_limit_bytes=56 << 20
        ),
        name="whole",
    )(byte_states, patch_of_byte.reshape(1, size), patch_first, moved, w_qkv, d_attn))


def solution(mesh):
    placed = (P("ctx", None), P("ctx"), P(), P(), P(None, None, "tp"), P("ctx", "tp"))
    return jax.shard_map(
        shards,
        mesh=mesh,
        in_specs=placed,
        out_specs=(P("ctx", "tp"), P("ctx", "tp")),
        check_vma=False,
    )
```

```python
import functools

import jax
import jax.numpy as jnp
from jax import lax
from jax.experimental import pallas as pl
from jax.experimental.pallas import tpu as pltpu
from jax.sharding import PartitionSpec as P

HD = 128
MESH = pl.DeviceIdType.MESH
VM = pl.BlockSpec(memory_space=pltpu.VMEM)


def remote(src, dst, send, recv, device):
    return pltpu.make_async_remote_copy(
        src_ref=src, dst_ref=dst, send_sem=send, recv_sem=recv, device_id=device, device_id_type=MESH
    )


def whole_kernel(
    n, tp, heads, rows, block,
    bytes_ref, pob_ref, first_ref, moved_ref, w_ref, d_ref,
    attn_ref, grad_ref,
    blk, came, pooled, wbuf, own3, qb, gb, kb, vb, ob, dqb, dkb, dvb, dka, dva,
    o_in, dq_in, dk_in, dv_in, part, own_part, lo_part, hi_part,
    w_sem, send_nb, recv_nb, send_kv, recv_kv, send_qg, recv_qg,
    send_dkv, recv_dkv, send_odq, recv_odq, send_rt, recv_rt, local_sem,
):
    groups = n // heads
    total = n * rows
    half = rows // 2
    scale = HD ** (-0.5)
    bf, f32 = jnp.bfloat16, jnp.float32
    me, mt = lax.axis_index("ctx"), lax.axis_index("tp")
    my_head, my_group = me // groups, lax.rem(me, groups)
    left, right = lax.rem(me + n - 1, n), lax.rem(me + 1, n)
    width = part.shape[2]

    def cols(head):
        return pl.ds(pl.multiple_of(head * HD, HD), HD)

    barrier = pltpu.get_barrier_semaphore()

    def greet(i, carry):
        peer = lax.rem(me + i, n)
        pl.semaphore_signal(barrier, inc=1, device_id=(peer, mt), device_id_type=MESH)
        return carry

    lax.fori_loop(1, n, greet, 0)
    for c in (me, left, right):
        for i in range(1, tp):
            pl.semaphore_signal(
                barrier, inc=1, device_id=(c, lax.rem(mt + i, tp)), device_id_type=MESH
            )
    loads = [pltpu.make_async_copy(w_ref.at[j], wbuf.at[j], w_sem.at[j]) for j in range(3)]
    for j in (1, 2, 0):
        loads[j].start()

    def plan(c):
        below = moved_ref[1, lax.rem(c + n - 1, n)]
        above = moved_ref[0, lax.rem(c + 1, n)]
        start = first_ref[c]
        end = jnp.where(c == n - 1, total, first_ref[lax.rem(c + 1, n)])
        return start, end, below, above, moved_ref[0, c], moved_ref[1, c]

    def numbers(c, rank):
        start, end, below, above, low, high = plan(c)
        return jnp.where(
            rank < below,
            start - below + rank,
            jnp.where(rank >= rows - above, end + rank - (rows - above), start + low + rank - below),
        )

    start, end, below, above, low, high = plan(me)
    count = end - start
    rank = lax.broadcasted_iota(jnp.int32, (2 * rows, 1), 0)
    own_rank = rank - 2 * half
    own_local = jnp.where((own_rank >= below) & (own_rank < rows - above), low + own_rank - below, -1)
    up = jnp.where(rank - half < high, count - high + rank - half, -1)
    wanted = jnp.where(rank < half, rank - half + low, jnp.where(rank < 2 * half, up, own_local))
    pob = pob_ref[...]
    member = (pob == wanted).astype(f32)
    lengths = jnp.maximum(jnp.sum(member, axis=1, keepdims=True), 1.0)
    means = (
        jnp.dot(member.astype(bf), bytes_ref[...], preferred_element_type=f32) / lengths
    ).astype(bf)
    blk[0] = means[:half]
    blk[1] = means[half : 2 * half]
    pl.semaphore_wait(barrier, n - 1 + 3 * (tp - 1))
    near = [
        remote(blk.at[i], came.at[i], send_nb.at[i], recv_nb.at[i], (peer, mt))
        for i, peer in enumerate((left, right))
    ]
    for copy in near:
        copy.start()

    def over_peers(make, wait=False):
        def body(i, carry):
            copy = make(i)
            if wait:
                copy.wait()
            else:
                copy.start()
            return carry

        lax.fori_loop(1, n, body, 0)

    def over_mates(make, wait=False):
        def body(i, carry):
            copy = make(i)
            if wait:
                copy.wait()
            else:
                copy.start()
            return carry

        lax.fori_loop(1, heads, body, 0)

    def to_peer(a, ref, out):
        def make(i):
            peer = lax.rem(me + i, n)
            return remote(
                ref.at[:, cols(peer // groups)], out.at[me], send_kv.at[a, i], recv_kv.at[a, i], (peer, mt)
            )

        return make

    def to_mate(a, ref, out):
        def make(i):
            head = lax.rem(my_head + i, heads)
            return remote(
                ref.at[:, cols(head)], out.at[my_head], send_qg.at[a, i], recv_qg.at[a, i],
                (head * groups + my_group, mt),
            )

        return make

    def back_peer(a, ref, out):
        def make(i):
            peer = lax.rem(me + i, n)
            return remote(
                ref.at[peer], out.at[my_group, :, cols(my_head)], send_dkv.at[a, i], recv_dkv.at[a, i],
                (peer, mt),
            )

        return make

    def back_mate(a, ref, out):
        def make(i):
            head = lax.rem(my_head + i, heads)
            return remote(
                ref.at[head], out.at[:, cols(my_head)], send_odq.at[a, i], recv_odq.at[a, i],
                (head * groups + my_group, mt),
            )

        return make

    mine = cols(my_head)
    send_g = to_mate(0, d_ref, gb)
    send_q = to_mate(1, own3.at[0], qb)
    send_k = to_peer(0, own3.at[1], kb)
    send_v = to_peer(1, own3.at[2], vb)
    over_mates(send_g)
    for copy in near:
        copy.wait()
    pooled[pl.ds(0, half)] = means[2 * half : 3 * half] + came[1]
    pooled[pl.ds(half, half)] = means[3 * half :] + came[0]
    for j, send in ((1, lambda: over_peers(send_k)), (2, lambda: over_peers(send_v)), (0, lambda: over_mates(send_q))):
        loads[j].wait()
        own3[j] = jnp.dot(pooled[...], wbuf[j], preferred_element_type=f32).astype(bf)
        send()
    own = [
        pltpu.make_async_copy(src, dst, local_sem.at[i])
        for i, (src, dst) in enumerate((
            (own3.at[1, :, mine], kb.at[me]), (own3.at[2, :, mine], vb.at[me]),
            (d_ref.at[:, mine], gb.at[my_head]), (own3.at[0, :, mine], qb.at[my_head]),
        ))
    ]
    for copy in own:
        copy.start()
    dka[...] = jnp.zeros_like(dka)
    dva[...] = jnp.zeros_like(dva)
    lane = lax.broadcasted_iota(jnp.int32, (1, total), 1)

    def number_keys(c, ids):
        return jnp.where((lane >= c * rows) & (lane < (c + 1) * rows), numbers(c, lane - c * rows), ids)

    kid = lax.fori_loop(0, n, number_keys, jnp.zeros((1, total), jnp.int32))
    for copy in own:
        copy.wait()
    over_mates(send_g, True)
    over_peers(send_k, True)
    over_peers(send_v, True)
    over_mates(send_q, True)

    over_last = (((1,), (1,)), ((), ()))
    over_first = (((0,), (0,)), ((), ()))
    back_o, back_q = back_mate(0, ob, o_in), back_mate(1, dqb, dq_in)
    row = lax.broadcasted_iota(jnp.int32, (rows, 1), 0)
    step_keys = 128 // rows if rows < 128 else 1
    send_dk, send_dv = back_peer(0, dkb, dk_in), back_peer(1, dvb, dv_in)

    def reach_of(b):
        if b < 0:
            return 0
        reach = min(n, (b + 1) * block * groups + 1)
        return min(n, -(-reach // step_keys) * step_keys)

    for b in reversed(range(heads // block)):
        lo = b * block
        reach, settled = reach_of(b), reach_of(b - 1)
        keys = reach * rows
        q = qb[pl.ds(lo, block)].reshape(block * rows, HD)
        g = gb[pl.ds(lo, block)].reshape(block * rows, HD)
        k = kb[pl.ds(0, reach)].reshape(keys, HD)
        v = vb[pl.ds(0, reach)].reshape(keys, HD)
        qid = jnp.concatenate([numbers((lo + j) * groups + my_group, row) for j in range(block)], axis=0)
        allowed = qid >= kid[:, :keys]
        score = lax.dot_general(q, k, over_last, preferred_element_type=f32) * scale
        score = jnp.where(allowed, score, -jnp.inf)
        top = jnp.max(score, axis=1, keepdims=True)
        e = jnp.exp(score - top)
        prob = e * (1.0 / jnp.sum(e, axis=1, keepdims=True))
        probs = prob.astype(bf)
        out = jnp.dot(probs, v, preferred_element_type=f32).astype(bf)
        delta = jnp.sum(g.astype(f32) * out.astype(f32), axis=1, keepdims=True)
        dprob = lax.dot_general(g, v, over_last, preferred_element_type=f32)
        dscore = (prob * (dprob - delta)).astype(bf)
        dq = (jnp.dot(dscore, k, preferred_element_type=f32) * scale).astype(bf)
        ob[pl.ds(lo, block)] = out.reshape(block, rows, HD)
        dqb[pl.ds(lo, block)] = dq.reshape(block, rows, HD)
        dka[pl.ds(0, keys)] += lax.dot_general(dscore, q, over_first, preferred_element_type=f32)
        dva[pl.ds(0, keys)] += lax.dot_general(probs, g, over_first, preferred_element_type=f32)
        for j in range(block):
            i = lax.rem(lo + j - my_head + heads, heads)

            @pl.when(i != 0)
            def _():
                back_o(i).start()
                back_q(i).start()

        if reach > settled:
            span = pl.ds(settled * rows, (reach - settled) * rows)
            shape = (reach - settled, rows, HD)
            dvb[pl.ds(settled, reach - settled)] = dva[span].astype(bf).reshape(shape)
            dkb[pl.ds(settled, reach - settled)] = (dka[span] * scale).astype(bf).reshape(shape)

            def send_back(peer, carry):
                i = lax.rem(peer - me + n, n)

                @pl.when(i != 0)
                def _():
                    send_dv(i).start()
                    send_dk(i).start()

                return carry

            lax.fori_loop(settled, reach, send_back, 0)

    own = [
        pltpu.make_async_copy(src, dst, local_sem.at[i])
        for i, (src, dst) in enumerate((
            (dkb.at[me], dk_in.at[my_group, :, mine]), (dvb.at[me], dv_in.at[my_group, :, mine]),
            (ob.at[my_head], o_in.at[:, mine]), (dqb.at[my_head], dq_in.at[:, mine]),
        ))
    ]
    for copy in own:
        copy.start()
    for copy in own:
        copy.wait()
    over_mates(back_o, True)
    attn_ref[...] = o_in[...]
    over_mates(back_q, True)
    partial = lax.dot_general(dq_in[...], wbuf[0], over_last, preferred_element_type=f32)
    for send, held, j in ((send_dv, dv_in, 2), (send_dk, dk_in, 1)):
        over_peers(send, True)
        summed = held[0].astype(f32)
        for i in range(1, groups):
            summed = summed + held[i].astype(f32)
        partial += lax.dot_general(summed.astype(bf), wbuf[j], over_last, preferred_element_type=f32)
    for t in range(tp):
        part[t] = partial[:, t * width : (t + 1) * width].astype(bf)
    edge_lo, edge_hi = pl.ds(0, half), pl.ds(rows - half, half)
    copies = []
    for i in range(1, tp):
        t = lax.rem(mt + i, tp)
        copies.append((part.at[t], own_part.at[mt], (me, t)))
    for i in range(tp):
        t = lax.rem(mt + i, tp)
        copies.append((part.at[t, edge_lo], hi_part.at[mt], (left, t)))
        copies.append((part.at[t, edge_hi], lo_part.at[mt], (right, t)))
    copies = [
        remote(src, dst, send_rt.at[i], recv_rt.at[i], peer) for i, (src, dst, peer) in enumerate(copies)
    ]
    for copy in copies:
        copy.start()
    kept = pltpu.make_async_copy(part.at[mt], own_part.at[mt], local_sem.at[0])
    kept.start()
    target = jnp.where(
        pob < low,
        half - low + pob,
        jnp.where(pob >= count - high, half + rows + pob - (count - high), half + below + pob - low),
    )
    chooser = (target == lax.broadcasted_iota(jnp.int32, (2 * rows, 1), 0)).astype(f32)
    sizes = jnp.maximum(jnp.sum(chooser, axis=1, keepdims=True), 1.0)
    kept.wait()
    for copy in copies:
        copy.wait()

    def over_tp(ref):
        value = ref[0].astype(f32)
        for i in range(1, tp):
            value = value + ref[i].astype(f32)
        return value

    returned = jnp.concatenate([over_tp(lo_part), over_tp(own_part), over_tp(hi_part)], axis=0)
    shares = (returned.astype(bf).astype(f32) / sizes).astype(bf)
    grad_ref[...] = lax.dot_general(
        chooser.astype(bf), shares, over_first, preferred_element_type=f32
    ).astype(bf)


def shards(byte_states, patch_of_byte, patch_first, moved, w_qkv, d_attn):
    n, tp = lax.axis_size("ctx"), lax.axis_size("tp")
    rows, feats = d_attn.shape
    size, model = byte_states.shape
    heads = feats // HD
    groups = n // heads
    total = n * rows
    half = rows // 2
    width = model // tp
    block = 2 if heads % 2 == 0 else 1
    bf, f32 = jnp.bfloat16, jnp.float32
    dma = pltpu.SemaphoreType.DMA
    smem = pl.BlockSpec(memory_space=pltpu.SMEM)
    return tuple(pl.pallas_call(
        functools.partial(whole_kernel, n, tp, heads, rows, block),
        out_shape=[
            jax.ShapeDtypeStruct((rows, feats), bf),
            jax.ShapeDtypeStruct((size, width), bf),
        ],
        in_specs=[VM, VM, smem, smem, pl.BlockSpec(memory_space=pl.ANY), VM],
        out_specs=[VM] * 2,
        scratch_shapes=[
            pltpu.VMEM((2, half, model), bf), pltpu.VMEM((2, half, model), bf),
            pltpu.VMEM((rows, model), bf), pltpu.VMEM(w_qkv.shape, bf), pltpu.VMEM((3, rows, feats), bf),
            pltpu.VMEM((heads, rows, HD), bf), pltpu.VMEM((heads, rows, HD), bf),
            pltpu.VMEM((n, rows, HD), bf), pltpu.VMEM((n, rows, HD), bf),
            pltpu.VMEM((heads, rows, HD), bf), pltpu.VMEM((heads, rows, HD), bf),
            pltpu.VMEM((n, rows, HD), bf), pltpu.VMEM((n, rows, HD), bf),
            pltpu.VMEM((total, HD), f32), pltpu.VMEM((total, HD), f32),
            pltpu.VMEM((rows, feats), bf), pltpu.VMEM((rows, feats), bf),
            pltpu.VMEM((groups, rows, feats), bf), pltpu.VMEM((groups, rows, feats), bf),
            pltpu.VMEM((tp, rows, width), bf), pltpu.VMEM((tp, rows, width), bf),
            pltpu.VMEM((tp, half, width), bf), pltpu.VMEM((tp, half, width), bf),
            dma((3,)), dma((2,)), dma((2,)), dma((2, n)), dma((2, n)), dma((2, heads)), dma((2, heads)),
            dma((2, n)), dma((2, n)), dma((2, heads)), dma((2, heads)),
            dma((3 * tp - 1,)), dma((3 * tp - 1,)), dma((4,)),
        ],
        compiler_params=pltpu.CompilerParams(
            collective_id=0, has_side_effects=True, vmem_limit_bytes=56 << 20
        ),
        name="whole",
    )(byte_states, patch_of_byte.reshape(1, size), patch_first, moved, w_qkv, d_attn))


def solution(mesh):
    placed = (P("ctx", None), P("ctx"), P(), P(), P(None, None, "tp"), P("ctx", "tp"))
    return jax.shard_map(
        shards,
        mesh=mesh,
        in_specs=placed,
        out_specs=(P("ctx", "tp"), P("ctx", "tp")),
        check_vma=False,
    )
```
